8 devices in a mesh: local: 2 (over z, y), data: 4 (over x, core).
Axes of the slice: x: 2, y: 2, z: 1, core: 2. Of those that a mesh axis runs over, the one named last changes fastest.
Arguments:
- x_in: bfloat16 [32768, 1280], P(('local', 'data'))
- grad_out: bfloat16 [32768, 1280], P(('local', 'data'))
- w_in: bfloat16 [3, 1280, 5120], P(None, ('local', 'data'))
- w_out: bfloat16 [3, 5120, 1280], P(None, ('local', 'data'))
Outputs:
- output 1: bfloat16 [32768, 1280], P(('local', 'data'))
- output 2: float32 [3, 1280, 5120], P(None, ('local', 'data'))
- output 3: float32 [3, 5120, 1280], P(None, ('local', 'data'))
- output 4: bfloat16 [32768, 1280], P(('local', 'data'))
All inputs are finite; a program needn't handle non-finite values.
Results may differ from the reference program's by a relative error of at most 0.0166592.
Values are sent between devices in bfloat16 or wider.
A program may use at most 1 GiB of HBM per device.

```python
import jax
import jax.numpy as jnp
from jax import lax

MODEL_DIM = 1280
FFN_DIM = 5120
LAYERS = 3
TOK_DEV = 4096
TOKENS = 32768
NORM_EPS = 1e-6


def setup_inputs(seed: int = 0) -> dict:
    key_list = jax.random.split(jax.random.key(seed), 4)
    x_in = jax.random.normal(key_list[0], (TOKENS, MODEL_DIM), jnp.float32)
    grad_out = jax.random.normal(key_list[1], (TOKENS, MODEL_DIM), jnp.float32) * TOKENS ** -0.5
    w_in = jax.random.normal(key_list[2], (LAYERS, MODEL_DIM, FFN_DIM), jnp.float32) * MODEL_DIM ** -0.5
    w_out = jax.random.normal(key_list[3], (LAYERS, FFN_DIM, MODEL_DIM), jnp.float32) * (1.5 * FFN_DIM ** -0.5)
    return {'x_in': x_in.astype(jnp.bfloat16), 'grad_out': grad_out.astype(jnp.bfloat16), 'w_in': w_in.astype(jnp.bfloat16), 'w_out': w_out.astype(jnp.bfloat16)}


def norm_rows(x_rows):
    x_wide = x_rows.astype(jnp.float32)
    inv_rms = lax.rsqrt(jnp.mean(x_wide * x_wide, axis=-1, keepdims=True) + NORM_EPS)
    return x_wide * inv_rms, inv_rms


def layer_inner(x_rows, w_in):
    unit_wide, inv_rms = norm_rows(x_rows)
    unit_rows = unit_wide.astype(jnp.bfloat16)
    pre_act = jnp.dot(unit_rows, w_in, preferred_element_type=jnp.float32).astype(jnp.bfloat16)
    gelu_val, gelu_back = jax.vjp(jax.nn.gelu, pre_act.astype(jnp.float32))
    return unit_wide, inv_rms, unit_rows, gelu_val.astype(jnp.bfloat16), gelu_back


def layer_forward(x_rows, w_in, w_out):
    hidden = layer_inner(x_rows, w_in)[3]
    branch = jnp.dot(hidden, w_out, preferred_element_type=jnp.float32)
    return (x_rows.astype(jnp.float32) + branch).astype(jnp.bfloat16)


def layer_backward(x_rows, grad_rows, w_in, w_out):
    unit_wide, inv_rms, unit_rows, hidden, gelu_back = layer_inner(x_rows, w_in)
    grad_hidden = jnp.dot(grad_rows, w_out.T, preferred_element_type=jnp.float32)
    grad_pre = gelu_back(grad_hidden)[0].astype(jnp.bfloat16)
    grad_w_out = jnp.dot(hidden.T, grad_rows, preferred_element_type=jnp.float32)
    grad_w_in = jnp.dot(unit_rows.T, grad_pre, preferred_element_type=jnp.float32)
    grad_unit = jnp.dot(grad_pre, w_in.T, preferred_element_type=jnp.float32)
    row_mean = jnp.mean(grad_unit * unit_wide, axis=-1, keepdims=True)
    grad_x = grad_rows.astype(jnp.float32) + inv_rms * (grad_unit - unit_wide * row_mean)
    return grad_x.astype(jnp.bfloat16), grad_w_in, grad_w_out


def block_grads(x_rows, grad_rows, w_in, w_out):
    def fwd_step(x_cur, weights):
        return layer_forward(x_cur, weights[0], weights[1]), x_cur

    x_last, saved_x = lax.scan(fwd_step, x_rows, (w_in, w_out))

    def bwd_step(grad_cur, step_items):
        grad_next, part_in, part_out = layer_backward(step_items[0], grad_cur, step_items[1], step_items[2])
        return grad_next, (part_in, part_out)

    grad_first, part_pair = lax.scan(bwd_step, grad_rows, (saved_x, w_in, w_out), reverse=True)
    return x_last, grad_first, part_pair[0], part_pair[1]


def reference(x_in, grad_out, w_in, w_out):
    blocks = TOKENS // TOK_DEV
    x_blocks = x_in.reshape(blocks, TOK_DEV, MODEL_DIM)
    grad_blocks = grad_out.reshape(blocks, TOK_DEV, MODEL_DIM)

    def block_step(acc_pair, step_items):
        x_last, grad_first, part_in, part_out = block_grads(step_items[0], step_items[1], w_in, w_out)
        return (acc_pair[0] + part_in, acc_pair[1] + part_out), (x_last, grad_first)

    start_acc = (jnp.zeros((LAYERS, MODEL_DIM, FFN_DIM), jnp.float32), jnp.zeros((LAYERS, FFN_DIM, MODEL_DIM), jnp.float32))
    acc_pair, row_outs = lax.scan(block_step, start_acc, (x_blocks, grad_blocks))
    return row_outs[0].reshape(TOKENS, MODEL_DIM), acc_pair[0], acc_pair[1], row_outs[1].reshape(TOKENS, MODEL_DIM)
```

```python
import functools

import jax
import jax.numpy as jnp
from jax import lax
from jax.experimental import pallas as pl
from jax.experimental.pallas import tpu as pltpu
from jax.sharding import Mesh, PartitionSpec as P


LAYERS = 3
D = 1280
F = 5120
T = 4096
NB = 4
NORM_EPS = 1e-6
C1 = 0.7978845608028654
C2 = C1 * 0.044715
LAST = (((1,), (1,)), ((), ()))
FIRST = (((0,), (0,)), ((), ()))
ANY = pl.BlockSpec(memory_space=pl.ANY)


def params(n):
    return pltpu.CompilerParams(vmem_limit_bytes=67000000, dimension_semantics=('arbitrary',) * n)


def norm_rows(x_wide):
    inv_rms = lax.rsqrt(jnp.mean(x_wide * x_wide, axis=-1, keepdims=True) + NORM_EPS)
    return x_wide * inv_rms, inv_rms


def gelu_fwd(a):
    t = jnp.tanh(a * (C1 + C2 * (a * a)))
    h = 0.5 * a
    return h + h * t


def gelu_both(a):
    a2 = a * a
    t = jnp.tanh(a * (C1 + C2 * a2))
    h = 0.5 * a
    slope = (0.5 + 0.5 * t) + (h * (1.0 - t * t)) * (C1 + (3.0 * C2) * a2)
    return h + h * t, slope


def load_weights(w1m, w1o, w2m, w2o, w1v, w2v, sems):
    c = lax.axis_index('c')
    r1 = D // 8
    r2 = F // 8
    copies = []
    for b in range(NB):
        for w1, w2, core in ((w1m, w2m, c), (w1o, w2o, 1 - c)):
            d = 2 * b + core
            copies.append(pltpu.make_async_copy(w1.at[pl.ds(b * r1, r1), :], w1v.at[pl.ds(pl.multiple_of(d * r1, r1), r1), :], sems.at[len(copies)]))
            copies.append(pltpu.make_async_copy(w2.at[pl.ds(b * r2, r2), :], w2v.at[pl.ds(pl.multiple_of(d * r2, r2), r2), :], sems.at[len(copies)]))
    for cp in copies:
        cp.start()
    for cp in copies:
        cp.wait()


WEIGHTS_VMEM = [pltpu.VMEM((D, F), jnp.bfloat16), pltpu.VMEM((F, D), jnp.bfloat16), pltpu.SemaphoreType.DMA((4 * NB,))]


def fwd_kernel(ch, x_ref, w1m, w1o, w2m, w2o, dep, o_ref, w1v, w2v, sems, u_s, acc):
    @pl.when(pl.program_id(0) == 0)
    def _():
        load_weights(w1m, w1o, w2m, w2o, w1v, w2v, sems)

    x_wide = x_ref[...].astype(jnp.float32)
    u_s[...] = norm_rows(x_wide)[0].astype(jnp.bfloat16)
    acc[...] = x_wide
    for j in range(F // ch):
        cols = pl.ds(j * ch, ch)
        a = jnp.dot(u_s[...], w1v[:, cols], preferred_element_type=jnp.float32).astype(jnp.bfloat16).astype(jnp.float32)
        s = gelu_fwd(a).astype(jnp.bfloat16)
        acc[...] += jnp.dot(s, w2v[cols, :], preferred_element_type=jnp.float32)
    o_ref[...] = acc[...].astype(jnp.bfloat16)


def fwd_call(x, w1m, w1o, w2m, w2o, dep, tm=512, ch=1024):
    row = pl.BlockSpec((tm, D), lambda i: (i, 0))
    return pl.pallas_call(
        functools.partial(fwd_kernel, ch), grid=(T // tm,), in_specs=[row] + [ANY] * 5, out_specs=row,
        out_shape=jax.ShapeDtypeStruct((T, D), jnp.bfloat16),
        scratch_shapes=WEIGHTS_VMEM + [pltpu.VMEM((tm, D), jnp.bfloat16), pltpu.VMEM((tm, D), jnp.float32)],
        compiler_params=params(1),
        cost_estimate=pl.CostEstimate(flops=4 * T * D * F, bytes_accessed=50000000, transcendentals=T * F),
        name='mlp_fwd')(x, w1m, w1o, w2m, w2o, dep)


def bwd_kernel(sub, full, x_ref, dy_ref, w1m, w1o, w2m, w2o, dep, s_ref, da_ref, ut_ref, *refs):
    w1v, w2v, sems, u_s = refs[-4:]
    i = pl.program_id(0)
    j = pl.program_id(1)

    @pl.when((i == 0) & (j == 0))
    def _():
        load_weights(w1m, w1o, w2m, w2o, w1v, w2v, sems)

    @pl.when(j == 0)
    def _():
        u = norm_rows(x_ref[...].astype(jnp.float32))[0].astype(jnp.bfloat16)
        u_s[...] = u
        ut_ref[...] = u.T

    ch = s_ref.shape[1]
    for k in range(ch // sub):
        cols = pl.ds(pl.multiple_of(j * ch + k * sub, sub), sub)
        a = jnp.dot(u_s[...], w1v[:, cols], preferred_element_type=jnp.float32).astype(jnp.bfloat16).astype(jnp.float32)
        ds = lax.dot_general(dy_ref[...], w2v[cols, :], LAST, preferred_element_type=jnp.float32)
        s, slope = gelu_both(a)
        s_ref[:, k * sub:(k + 1) * sub] = s.astype(jnp.bfloat16)
        da_ref[:, k * sub:(k + 1) * sub] = (slope * ds).astype(jnp.bfloat16)
    if not full:
        return
    dx_ref, acc = refs[:2]
    cols = pl.ds(pl.multiple_of(j * ch, ch), ch)
    du = lax.dot_general(da_ref[...], w1v[:, cols], LAST, preferred_element_type=jnp.float32)

    @pl.when(j == 0)
    def _():
        acc[...] = du

    @pl.when(j > 0)
    def _():
        acc[...] += du

    @pl.when(j == pl.num_programs(1) - 1)
    def _():
        dx_ref[...] = norm_back(x_ref[...], dy_ref[...], acc[...])


def norm_back(x, dy, du):
    v, inv_rms = norm_rows(x.astype(jnp.float32))
    m = jnp.mean(du * v, axis=-1, keepdims=True)
    return (dy.astype(jnp.float32) + inv_rms * (du - v * m)).astype(jnp.bfloat16)


def bwd_call(x, dy, w1m, w1o, w2m, w2o, dep, full=True, tm=512, ch=2560, sub=512):
    row = pl.BlockSpec((tm, D), lambda i, j: (i, 0))
    hid = pl.BlockSpec((tm, ch), lambda i, j: (i, j))
    n = int(full)
    return pl.pallas_call(
        functools.partial(bwd_kernel, sub, full), grid=(T // tm, F // ch), in_specs=[row, row] + [ANY] * 5,
        out_specs=[hid, hid, pl.BlockSpec((D, tm), lambda i, j: (0, i))] + [row] * n,
        out_shape=[jax.ShapeDtypeStruct((T, F), jnp.bfloat16)] * 2 + [jax.ShapeDtypeStruct((D, T), jnp.bfloat16)] + [jax.ShapeDtypeStruct((T, D), jnp.bfloat16)] * n,
        scratch_shapes=[pltpu.VMEM((tm, D), jnp.float32)] * n + WEIGHTS_VMEM + [pltpu.VMEM((tm, D), jnp.bfloat16)],
        compiler_params=params(2),
        cost_estimate=pl.CostEstimate(flops=(4 + 2 * n) * T * D * F, bytes_accessed=150000000, transcendentals=T * F),
        name='mlp_bwd')(x, dy, w1m, w1o, w2m, w2o, dep)


def du_kernel(x_ref, dy_ref, da_ref, w1m, w1o, dep, dx_ref, w1v, sems):
    @pl.when(pl.program_id(0) == 0)
    def _():
        c = lax.axis_index('c')
        r = D // 8
        copies = []
        for b in range(NB):
            for w1, core in ((w1m, c), (w1o, 1 - c)):
                d = 2 * b + core
                copies.append(pltpu.make_async_copy(w1.at[pl.ds(b * r, r), :], w1v.at[pl.ds(pl.multiple_of(d * r, r), r), :], sems.at[len(copies)]))
        for cp in copies:
            cp.start()
        for cp in copies:
            cp.wait()

    du = lax.dot_general(da_ref[...], w1v[...], LAST, preferred_element_type=jnp.float32)
    dx_ref[...] = norm_back(x_ref[...], dy_ref[...], du)


def du_call(x, dy, da, w1m, w1o, dep, tm=512):
    row = pl.BlockSpec((tm, D), lambda i: (i, 0))
    return pl.pallas_call(
        du_kernel, grid=(T // tm,), in_specs=[row, row, pl.BlockSpec((tm, F), lambda i: (i, 0))] + [ANY] * 3, out_specs=row,
        out_shape=jax.ShapeDtypeStruct((T, D), jnp.bfloat16),
        scratch_shapes=[pltpu.VMEM((D, F), jnp.bfloat16), pltpu.SemaphoreType.DMA((2 * NB,))],
        compiler_params=params(1),
        cost_estimate=pl.CostEstimate(flops=2 * T * D * F, bytes_accessed=80000000, transcendentals=0),
        name='grad_x')(x, dy, da, w1m, w1o, dep)


def wout_kernel(cs, s_ref, dy_ref, dep, *refs):
    v = lax.dot_general(s_ref[...], dy_ref[...], FIRST, preferred_element_type=jnp.float32)
    refs[-1][...] = v + refs[0][...] if len(refs) == 2 else v


def wout_call(s, dy, core, dep, recv=None):
    extra = [] if recv is None else [recv]
    bm = F // 8
    blk = pl.BlockSpec((bm, D), lambda b, cs: (b, 0))
    spec = pltpu.PrefetchScalarGridSpec(
        num_scalar_prefetch=1, grid=(NB,),
        in_specs=[pl.BlockSpec((T, bm), lambda b, cs: (0, 2 * b + cs[0])), pl.BlockSpec((T, D), lambda b, cs: (0, 0), pipeline_mode=pl.Buffered(1)), ANY] + [blk] * len(extra),
        out_specs=blk)
    return pl.pallas_call(
        wout_kernel, grid_spec=spec, out_shape=jax.ShapeDtypeStruct((F // 2, D), jnp.float32), compiler_params=params(1),
        cost_estimate=pl.CostEstimate(flops=T * D * F, bytes_accessed=50000000, transcendentals=0),
        name='grad_w_out')(core, s, dy, dep, *extra)


def win_kernel(cs, ut, da_ref, dep, *refs):
    o_ref, lhs, sems = refs[-3:]

    @pl.when(pl.program_id(0) == 0)
    def _():
        r = D // 8
        copies = [pltpu.make_async_copy(ut.at[pl.ds(pl.multiple_of((2 * b + cs[0]) * r, r), r), :], lhs.at[pl.ds(b * r, r), :], sems.at[b]) for b in range(NB)]
        for cp in copies:
            cp.start()
        for cp in copies:
            cp.wait()

    v = jnp.dot(lhs[...], da_ref[...], preferred_element_type=jnp.float32)
    o_ref[...] = v + refs[0][...] if len(refs) == 4 else v


def win_call(ut, da, core, dep, recv=None, bn=512):
    extra = [] if recv is None else [recv]
    blk = pl.BlockSpec((D // 2, bn), lambda n, cs: (0, n))
    spec = pltpu.PrefetchScalarGridSpec(
        num_scalar_prefetch=1, grid=(F // bn,),
        in_specs=[ANY, pl.BlockSpec((T, bn), lambda n, cs: (0, n)), ANY] + [blk] * len(extra), out_specs=blk,
        scratch_shapes=[pltpu.VMEM((D // 2, T), jnp.bfloat16), pltpu.SemaphoreType.DMA((NB,))])
    return pl.pallas_call(
        win_kernel, grid_spec=spec, out_shape=jax.ShapeDtypeStruct((D // 2, F), jnp.float32), compiler_params=params(1),
        cost_estimate=pl.CostEstimate(flops=T * D * F, bytes_accessed=50000000, transcendentals=0),
        name='grad_w_in')(core, ut, da, dep, *extra)


SWAP = [(0, 1), (1, 0)]
CHIPS = ('y', 'x')
ALL = ('y', 'x', 'c')


def swap(v):
    return lax.ppermute(v, 'c', SWAP)


def place(stack, item, l):
    return lax.dynamic_update_slice(stack, item[None], (l, 0, 0))


def solution(mesh):
    fine = Mesh(mesh.devices.reshape(2, 2, 2), ALL)

    def device_step(x_rows, grad_rows, w_in, w_out):
        me = lax.axis_index('c').astype(jnp.int32)[None]
        other = 1 - me

        def gather(l, tok):
            p1, p2 = w_in[l], w_out[l]
            if tok:
                p1, p2 = lax.optimization_barrier((p1, p2) + tok)[:2]
            g1 = lax.all_gather(p1, CHIPS, axis=0, tiled=True)
            g2 = lax.all_gather(p2, CHIPS, axis=0, tiled=True)
            return g1, g2

        kept = [gather(0, ())]
        xs = [x_rows]
        for l in range(LAYERS - 1):
            kept.append(gather(l + 1, kept[-1]))
            w1, w2 = kept[l]
            w1o, w2o = swap(w1), swap(w2)
            xs.append(fwd_call(xs[-1], w1, w1o, w2, w2o, x_rows))
        grad = grad_rows
        tok = xs[-1]
        out_in = jnp.zeros((LAYERS, D // 8, F), jnp.float32)
        out_out = jnp.zeros((LAYERS, F // 8, D), jnp.float32)
        for l in reversed(range(LAYERS)):
            w1, w2 = kept[l]
            if l < LAYERS - 1:
                w1, w2 = lax.optimization_barrier((w1, w2, grad))[:2]
            w1o = swap(w1)
            s, da, ut, *rest = bwd_call(xs[l], grad, w1, w1o, w2, swap(w2), tok, full=l > 0)
            send_out = wout_call(s, grad, other, tok)
            send_in = win_call(ut, da, other, send_out)
            recv_in = swap(send_in)
            part_out = wout_call(s, grad, me, send_in, swap(send_out))
            out_out = place(out_out, lax.psum_scatter(part_out, CHIPS, scatter_dimension=0, tiled=True), l)
            part_in = win_call(ut, da, me, part_out, recv_in)
            out_in = place(out_in, lax.psum_scatter(part_in, CHIPS, scatter_dimension=0, tiled=True), l)
            tok = part_in
            grad = rest[0] if rest else du_call(xs[l], grad, da, w1, w1o, tok)
        w1, w2 = lax.optimization_barrier(kept[-1] + (send_in,))[:2]
        x_out = fwd_call(xs[-1], w1, swap(w1), w2, swap(w2), tok)
        return x_out, out_in, out_out, grad

    row = P(ALL, None)
    wt = P(None, ALL, None)
    return jax.shard_map(device_step, mesh=fine, in_specs=(row, row, wt, wt), out_specs=(row, wt, wt, row), check_vma=False)
```

```python
import functools

import jax
import jax.numpy as jnp
from jax import lax
from jax.experimental import pallas as pl
from jax.experimental.pallas import tpu as pltpu
from jax.sharding import Mesh, PartitionSpec as P


LAYERS = 3
D = 1280
F = 5120
T = 4096
NB = 4
NORM_EPS = 1e-6
C1 = 0.7978845608028654
C2 = C1 * 0.044715
LAST = (((1,), (1,)), ((), ()))
FIRST = (((0,), (0,)), ((), ()))
ANY = pl.BlockSpec(memory_space=pl.ANY)


def params(n):
    return pltpu.CompilerParams(vmem_limit_bytes=67000000, dimension_semantics=('arbitrary',) * n)


def norm_rows(x_wide):
    inv_rms = lax.rsqrt(jnp.mean(x_wide * x_wide, axis=-1, keepdims=True) + NORM_EPS)
    return x_wide * inv_rms, inv_rms


def gelu_fwd(a):
    t = jnp.tanh(a * (C1 + C2 * (a * a)))
    h = 0.5 * a
    return h + h * t


def gelu_both(a):
    a2 = a * a
    t = jnp.tanh(a * (C1 + C2 * a2))
    h = 0.5 * a
    slope = (0.5 + 0.5 * t) + (h * (1.0 - t * t)) * (C1 + (3.0 * C2) * a2)
    return h + h * t, slope


def load_weights(w1m, w1o, w2m, w2o, w1v, w2v, sems):
    c = lax.axis_index('c')
    r1 = D // 8
    r2 = F // 8
    copies = []
    for b in range(NB):
        for w1, w2, core in ((w1m, w2m, c), (w1o, w2o, 1 - c)):
            d = 2 * b + core
            copies.append(pltpu.make_async_copy(w1.at[pl.ds(b * r1, r1), :], w1v.at[pl.ds(pl.multiple_of(d * r1, r1), r1), :], sems.at[len(copies)]))
            copies.append(pltpu.make_async_copy(w2.at[pl.ds(b * r2, r2), :], w2v.at[pl.ds(pl.multiple_of(d * r2, r2), r2), :], sems.at[len(copies)]))
    for cp in copies:
        cp.start()
    for cp in copies:
        cp.wait()


WEIGHTS_VMEM = [pltpu.VMEM((D, F), jnp.bfloat16), pltpu.VMEM((F, D), jnp.bfloat16), pltpu.SemaphoreType.DMA((4 * NB,))]


def fwd_kernel(ch, x_ref, w1m, w1o, w2m, w2o, dep, o_ref, w1v, w2v, sems, u_s, acc):
    @pl.when(pl.program_id(0) == 0)
    def _():
        load_weights(w1m, w1o, w2m, w2o, w1v, w2v, sems)

    x_wide = x_ref[...].astype(jnp.float32)
    u_s[...] = norm_rows(x_wide)[0].astype(jnp.bfloat16)
    acc[...] = x_wide

    def hidden(j):
        return jnp.dot(u_s[...], w1v[:, pl.ds(j * ch, ch)], preferred_element_type=jnp.float32).astype(jnp.bfloat16)

    n = F // ch
    held = hidden(0)
    for j in range(n):
        ahead = hidden(j + 1) if j + 1 < n else None
        s = gelu_fwd(held.astype(jnp.float32)).astype(jnp.bfloat16)
        acc[...] += jnp.dot(s, w2v[pl.ds(j * ch, ch), :], preferred_element_type=jnp.float32)
        held = ahead
    o_ref[...] = acc[...].astype(jnp.bfloat16)


def fwd_call(x, w1m, w1o, w2m, w2o, dep, tm=512, ch=1280):
    row = pl.BlockSpec((tm, D), lambda i: (i, 0))
    return pl.pallas_call(
        functools.partial(fwd_kernel, ch), grid=(T // tm,), in_specs=[row] + [ANY] * 5, out_specs=row,
        out_shape=jax.ShapeDtypeStruct((T, D), jnp.bfloat16),
        scratch_shapes=WEIGHTS_VMEM + [pltpu.VMEM((tm, D), jnp.bfloat16), pltpu.VMEM((tm, D), jnp.float32)],
        compiler_params=params(1),
        cost_estimate=pl.CostEstimate(flops=4 * T * D * F, bytes_accessed=50000000, transcendentals=T * F),
        name='mlp_fwd')(x, w1m, w1o, w2m, w2o, dep)


def bwd_kernel(sub, full, x_ref, dy_ref, w1m, w1o, w2m, w2o, dep, s_ref, da_ref, ut_ref, *refs):
    w1v, w2v, sems, u_s = refs[-4:]
    i = pl.program_id(0)
    j = pl.program_id(1)

    @pl.when((i == 0) & (j == 0))
    def _():
        load_weights(w1m, w1o, w2m, w2o, w1v, w2v, sems)

    @pl.when(j == 0)
    def _():
        u = norm_rows(x_ref[...].astype(jnp.float32))[0].astype(jnp.bfloat16)
        u_s[...] = u
        ut_ref[...] = u.T

    ch = s_ref.shape[1]
    n = ch // sub
    if full:
        dx_ref, acc = refs[:2]

        @pl.when(j == 0)
        def _():
            acc[...] = jnp.zeros_like(acc)

    def cols(k, width):
        return pl.ds(pl.multiple_of(j * ch + k * sub, sub), width)

    def dots(k):
        a = jnp.dot(u_s[...], w1v[:, cols(k, sub)], preferred_element_type=jnp.float32).astype(jnp.bfloat16).astype(jnp.float32)
        return a, lax.dot_general(dy_ref[...], w2v[cols(k, sub), :], LAST, preferred_element_type=jnp.float32)

    def elementwise(k, a, ds):
        s, slope = gelu_both(a)
        s_ref[:, k * sub:(k + 1) * sub] = s.astype(jnp.bfloat16)
        da_ref[:, k * sub:(k + 1) * sub] = (slope * ds).astype(jnp.bfloat16)

    def add_du(k, width):
        acc[...] += lax.dot_general(da_ref[:, k * sub:k * sub + width], w1v[:, cols(k, width)], LAST, preferred_element_type=jnp.float32)

    held = dots(0)
    for k in range(1, n + 1):
        ahead = dots(k) if k < n else None
        elementwise(k - 1, *held)
        held = ahead
    if not full:
        return
    add_du(0, ch)

    @pl.when(j == pl.num_programs(1) - 1)
    def _():
        dx_ref[...] = norm_back(x_ref[...], dy_ref[...], acc[...])


def norm_back(x, dy, du):
    v, inv_rms = norm_rows(x.astype(jnp.float32))
    m = jnp.mean(du * v, axis=-1, keepdims=True)
    return (dy.astype(jnp.float32) + inv_rms * (du - v * m)).astype(jnp.bfloat16)


def bwd_call(x, dy, w1m, w1o, w2m, w2o, dep, full=True, tm=512, ch=2560, sub=512):
    row = pl.BlockSpec((tm, D), lambda i, j: (i, 0))
    hid = pl.BlockSpec((tm, ch), lambda i, j: (i, j))
    n = int(full)
    return pl.pallas_call(
        functools.partial(bwd_kernel, sub, full), grid=(T // tm, F // ch), in_specs=[row, row] + [ANY] * 5,
        out_specs=[hid, hid, pl.BlockSpec((D, tm), lambda i, j: (0, i))] + [row] * n,
        out_shape=[jax.ShapeDtypeStruct((T, F), jnp.bfloat16)] * 2 + [jax.ShapeDtypeStruct((D, T), jnp.bfloat16)] + [jax.ShapeDtypeStruct((T, D), jnp.bfloat16)] * n,
        scratch_shapes=[pltpu.VMEM((tm, D), jnp.float32)] * n + WEIGHTS_VMEM + [pltpu.VMEM((tm, D), jnp.bfloat16)],
        compiler_params=params(2),
        cost_estimate=pl.CostEstimate(flops=(4 + 2 * n) * T * D * F, bytes_accessed=150000000, transcendentals=T * F),
        name='mlp_bwd')(x, dy, w1m, w1o, w2m, w2o, dep)


def du_kernel(x_ref, dy_ref, da_ref, w1m, w1o, dep, dx_ref, w1v, sems):
    @pl.when(pl.program_id(0) == 0)
    def _():
        c = lax.axis_index('c')
        r = D // 8
        copies = []
        for b in range(NB):
            for w1, core in ((w1m, c), (w1o, 1 - c)):
                d = 2 * b + core
                copies.append(pltpu.make_async_copy(w1.at[pl.ds(b * r, r), :], w1v.at[pl.ds(pl.multiple_of(d * r, r), r), :], sems.at[len(copies)]))
        for cp in copies:
            cp.start()
        for cp in copies:
            cp.wait()

    du = lax.dot_general(da_ref[...], w1v[...], LAST, preferred_element_type=jnp.float32)
    dx_ref[...] = norm_back(x_ref[...], dy_ref[...], du)


def du_call(x, dy, da, w1m, w1o, dep, tm=512):
    row = pl.BlockSpec((tm, D), lambda i: (i, 0))
    return pl.pallas_call(
        du_kernel, grid=(T // tm,), in_specs=[row, row, pl.BlockSpec((tm, F), lambda i: (i, 0))] + [ANY] * 3, out_specs=row,
        out_shape=jax.ShapeDtypeStruct((T, D), jnp.bfloat16),
        scratch_shapes=[pltpu.VMEM((D, F), jnp.bfloat16), pltpu.SemaphoreType.DMA((2 * NB,))],
        compiler_params=params(1),
        cost_estimate=pl.CostEstimate(flops=2 * T * D * F, bytes_accessed=80000000, transcendentals=0),
        name='grad_x')(x, dy, da, w1m, w1o, dep)


def wout_kernel(cs, s_ref, dy_ref, dep, *refs):
    v = lax.dot_general(s_ref[...], dy_ref[...], FIRST, preferred_element_type=jnp.float32)
    refs[-1][...] = v + refs[0][...] if len(refs) == 2 else v


def wout_call(s, dy, core, dep, recv=None):
    extra = [] if recv is None else [recv]
    bm = F // 8
    blk = pl.BlockSpec((bm, D), lambda b, cs: (b, 0))
    spec = pltpu.PrefetchScalarGridSpec(
        num_scalar_prefetch=1, grid=(NB,),
        in_specs=[pl.BlockSpec((T, bm), lambda b, cs: (0, 2 * b + cs[0])), pl.BlockSpec((T, D), lambda b, cs: (0, 0), pipeline_mode=pl.Buffered(1)), ANY] + [blk] * len(extra),
        out_specs=blk)
    return pl.pallas_call(
        wout_kernel, grid_spec=spec, out_shape=jax.ShapeDtypeStruct((F // 2, D), jnp.float32), compiler_params=params(1),
        cost_estimate=pl.CostEstimate(flops=T * D * F, bytes_accessed=50000000, transcendentals=0),
        name='grad_w_out')(core, s, dy, dep, *extra)


def win_kernel(cs, ut, da_ref, dep, *refs):
    o_ref, lhs, sems = refs[-3:]

    @pl.when(pl.program_id(0) == 0)
    def _():
        r = D // 8
        copies = [pltpu.make_async_copy(ut.at[pl.ds(pl.multiple_of((2 * b + cs[0]) * r, r), r), :], lhs.at[pl.ds(b * r, r), :], sems.at[b]) for b in range(NB)]
        for cp in copies:
            cp.start()
        for cp in copies:
            cp.wait()

    v = jnp.dot(lhs[...], da_ref[...], preferred_element_type=jnp.float32)
    o_ref[...] = v + refs[0][...] if len(refs) == 4 else v


def win_call(ut, da, core, dep, recv=None, bn=512):
    extra = [] if recv is None else [recv]
    blk = pl.BlockSpec((D // 2, bn), lambda n, cs: (0, n))
    spec = pltpu.PrefetchScalarGridSpec(
        num_scalar_prefetch=1, grid=(F // bn,),
        in_specs=[ANY, pl.BlockSpec((T, bn), lambda n, cs: (0, n)), ANY] + [blk] * len(extra), out_specs=blk,
        scratch_shapes=[pltpu.VMEM((D // 2, T), jnp.bfloat16), pltpu.SemaphoreType.DMA((NB,))])
    return pl.pallas_call(
        win_kernel, grid_spec=spec, out_shape=jax.ShapeDtypeStruct((D // 2, F), jnp.float32), compiler_params=params(1),
        cost_estimate=pl.CostEstimate(flops=T * D * F, bytes_accessed=50000000, transcendentals=0),
        name='grad_w_in')(core, ut, da, dep, *extra)


SWAP = [(0, 1), (1, 0)]
CHIPS = ('y', 'x')
ALL = ('y', 'x', 'c')


def swap(v):
    return lax.ppermute(v, 'c', SWAP)


def place(stack, item, l):
    return lax.dynamic_update_slice(stack, item[None], (l, 0, 0))


def solution(mesh):
    fine = Mesh(mesh.devices.reshape(2, 2, 2), ALL)

    def device_step(x_rows, grad_rows, w_in, w_out):
        me = lax.axis_index('c').astype(jnp.int32)[None]
        other = 1 - me

        def gather(l, tok):
            p1, p2 = w_in[l], w_out[l]
            if tok:
                p1, p2 = lax.optimization_barrier((p1, p2) + tok)[:2]
            g1 = lax.all_gather(p1, CHIPS, axis=0, tiled=True)
            g2 = lax.all_gather(p2, CHIPS, axis=0, tiled=True)
            return g1, g2

        kept = [gather(0, ())]
        first = swap(kept[0][0])
        xs = [x_rows]
        for l in range(LAYERS - 1):
            kept.append(gather(l + 1, kept[-1] + ((first,) if l == 0 else ())))
            w1, w2 = kept[l]
            w1o, w2o = swap(w1) if l else first, swap(w2)
            xs.append(fwd_call(xs[-1], w1, w1o, w2, w2o, x_rows))
        grad = grad_rows
        tok = xs[-1]
        out_in = jnp.zeros((LAYERS, D // 8, F), jnp.float32)
        out_out = jnp.zeros((LAYERS, F // 8, D), jnp.float32)
        for l in reversed(range(LAYERS)):
            w1, w2 = kept[l]
            if l < LAYERS - 1:
                w1, w2 = lax.optimization_barrier((w1, w2, grad))[:2]
            w1o = swap(w1)
            s, da, ut, *rest = bwd_call(xs[l], grad, w1, w1o, w2, swap(w2), tok, full=l > 0)
            send_out = wout_call(s, grad, other, tok)
            send_in = win_call(ut, da, other, send_out)
            recv_in = swap(send_in)
            part_out = wout_call(s, grad, me, send_in, swap(send_out))
            out_out = place(out_out, lax.psum_scatter(part_out, CHIPS, scatter_dimension=0, tiled=True), l)
            part_in = win_call(ut, da, me, part_out, recv_in)
            out_in = place(out_in, lax.psum_scatter(part_in, CHIPS, scatter_dimension=0, tiled=True), l)
            tok = part_in
            grad = rest[0] if rest else du_call(xs[l], grad, da, w1, w1o, tok)
        w1, w2 = lax.optimization_barrier(kept[-1] + (send_in,))[:2]
        x_out = fwd_call(xs[-1], w1, swap(w1), w2, swap(w2), tok)
        return x_out, out_in, out_out, grad

    row = P(ALL, None)
    wt = P(None, ALL, None)
    return jax.shard_map(device_step, mesh=fine, in_specs=(row, row, wt, wt), out_specs=(row, wt, wt, row), check_vma=False)
```
